32 devices in a mesh: batch: 8 (over y, x, core), cols: 4 (over z).
Axes of the slice: x: 2, y: 2, z: 4, core: 2. Of those that a mesh axis runs over, the one named last changes fastest.
Arguments:
- grad_up: float32 [8, 1024, 4096], P('batch', None, 'cols'), may hold values from -0.875 to 0.875
- grad_down: float32 [8, 4096, 1024], P('batch', 'cols'), may hold values from -0.875 to 0.875
- grad_query: float32 [8, 1024, 1024], P('batch', None, 'cols'), may hold values from -0.875 to 0.875
- grad_key: float32 [8, 1024, 1024], P('batch', None, 'cols'), may hold values from -0.875 to 0.875
- grad_value: float32 [8, 1024, 1024], P('batch', None, 'cols'), may hold values from -0.875 to 0.875
- grad_mixed: float32 [8, 1024, 1024], P('batch', 'cols'), may hold values from -0.875 to 0.875
- grad_norm: float32 [8, 1024], P('batch'), may hold values from -8 to 8
- weight_up: float32 [1024, 4096], P('batch', 'cols'), may hold values from -0.1875 to 0.1875
- weight_down: float32 [4096, 1024], P('cols', 'batch'), may hold values from -0.09375 to 0.09375
- weight_query: float32 [1024, 1024], P('batch', 'cols'), may hold values from -0.1875 to 0.1875
- weight_key: float32 [1024, 1024], P('batch', 'cols'), may hold values from -0.1875 to 0.1875
- weight_value: float32 [1024, 1024], P('batch', 'cols'), may hold values from -0.1875 to 0.1875
- weight_mixed: float32 [1024, 1024], P('cols', 'batch'), may hold values from -0.1875 to 0.1875
- weight_norm: float32 [1024], P('batch'), may hold values from 0.25 to 1.75
- moment_up: float32 [1024, 4096], P('batch', 'cols'), may hold values from -1.75 to 1.75
- moment_down: float32 [4096, 1024], P('cols', 'batch'), may hold values from -1.75 to 1.75
- moment_query: float32 [1024, 1024], P('batch', 'cols'), may hold values from -1.75 to 1.75
- moment_key: float32 [1024, 1024], P('batch', 'cols'), may hold values from -1.75 to 1.75
- moment_value: float32 [1024, 1024], P('batch', 'cols'), may hold values from -1.75 to 1.75
- moment_mixed: float32 [1024, 1024], P('cols', 'batch'), may hold values from -1.75 to 1.75
- moment_norm: float32 [1024], P('batch'), may hold values from -1.75 to 1.75
Outputs:
- copy_up: bfloat16 [1024, 4096], P(None, 'cols')
- copy_down: bfloat16 [4096, 1024], P('cols')
- copy_query: bfloat16 [1024, 1024], P(None, 'cols')
- copy_key: bfloat16 [1024, 1024], P(None, 'cols')
- copy_value: bfloat16 [1024, 1024], P(None, 'cols')
- copy_mixed: bfloat16 [1024, 1024], P('cols')
- copy_norm: bfloat16 [1024], replicated
- new_up: float32 [1024, 4096], P('batch', 'cols')
- new_down: float32 [4096, 1024], P('cols', 'batch')
- new_query: float32 [1024, 1024], P('batch', 'cols')
- new_key: float32 [1024, 1024], P('batch', 'cols')
- new_value: float32 [1024, 1024], P('batch', 'cols')
- new_mixed: float32 [1024, 1024], P('cols', 'batch')
- new_norm: float32 [1024], P('batch')
- state_new_up: float32 [1024, 4096], P('batch', 'cols')
- state_new_down: float32 [4096, 1024], P('cols', 'batch')
- state_new_query: float32 [1024, 1024], P('batch', 'cols')
- state_new_key: float32 [1024, 1024], P('batch', 'cols')
- state_new_value: float32 [1024, 1024], P('batch', 'cols')
- state_new_mixed: float32 [1024, 1024], P('cols', 'batch')
- state_new_norm: float32 [1024], P('batch')
The draws below stay inside these ranges and needn't reach their ends.
All inputs are finite; a program needn't handle non-finite values.
Results may differ from the reference program's by a relative error of at most 0.008.
Values may be sent and summed in bfloat16 or wider, within the bound.
No kernel may reach another device: no remote copies, remote signals or barrier semaphores. Data moves between devices by JAX's collectives and lax.ppermute only.
A program may use at most 64 MiB of HBM per device.

```python
import jax
import jax.numpy as jnp

WIDTH = 1024
INNER = 4096
ATTN = 1024
REPLICAS = 8


def spiked(entries, rng, source, target, blocks, factor):
    owner, partner = [(jnp.arange(entries.shape[dim]) // (entries.shape[dim] // blocks)).reshape([-1 if axis == dim else 1 for axis in range(entries.ndim)]) for dim in (source, target)]
    chosen = jax.random.permutation(rng, blocks)[partner]
    strong = (owner == chosen) | (owner == (partner + blocks // 2) % blocks)
    return jnp.where(strong, factor * entries, entries)


def steps_of(rng, dims, cuts, smallest, top_value):
    level = 1.0
    for dim, parts in cuts:
        heights = jax.random.uniform(jax.random.fold_in(jax.random.fold_in(rng, 6), dim), (parts,), jnp.float32, smallest / len(cuts), top_value / len(cuts))
        level = level * jnp.repeat(jnp.exp(heights), dims[dim] // parts).reshape((-1,) + (1,) * (len(dims) - 1 - dim))
    return level


def centred(key, shape, scale, bound, pieces=(), kind=jnp.bfloat16):
    loudness = steps_of(key, shape, pieces, -0.22, 0.18) if pieces else 1.0
    drawn = jax.random.normal(key, shape, jnp.float32) * scale * loudness
    return jnp.minimum(jnp.maximum(drawn, -bound), bound).astype(kind)


def bell_draw_with(own_key, shape, deviation, most, split, heavy, kind=jnp.bfloat16):
    array = deviation * jax.random.normal(own_key, shape, jnp.float32)
    if split:
        array = array * steps_of(own_key, shape, split, -0.22, 0.18)
    return jnp.clip(spiked(array, jax.random.fold_in(own_key, 3), *heavy), -most, most).astype(kind)


def setup_inputs(seed: int = 0) -> dict:
    arg_keys = jax.random.split(jax.random.key(seed), 22)
    return {
        "grad_up": bell_draw_with(arg_keys[0], (REPLICAS, WIDTH, INNER), 0.1, 0.875, ((0, 8), (2, 4)), (0, 1, 8, 2.0), jnp.float32),
        "grad_down": bell_draw_with(arg_keys[1], (REPLICAS, INNER, WIDTH), 0.1, 0.875, ((0, 8), (1, 4)), (0, 2, 8, 2.0), jnp.float32),
        "grad_query": bell_draw_with(arg_keys[2], (REPLICAS, WIDTH, ATTN), 0.1, 0.875, ((0, 8), (2, 4)), (0, 1, 8, 2.0), jnp.float32),
        "grad_key": bell_draw_with(arg_keys[3], (REPLICAS, WIDTH, ATTN), 0.1, 0.875, ((0, 8), (2, 4)), (0, 1, 8, 2.0), jnp.float32),
        "grad_value": bell_draw_with(arg_keys[4], (REPLICAS, WIDTH, ATTN), 0.1, 0.875, ((0, 8), (2, 4)), (0, 1, 8, 2.0), jnp.float32),
        "grad_mixed": bell_draw_with(arg_keys[5], (REPLICAS, ATTN, WIDTH), 0.1, 0.875, ((0, 8), (1, 4)), (0, 2, 8, 2.0), jnp.float32),
        "grad_norm": bell_draw_with(arg_keys[6], (REPLICAS, WIDTH), 1.0, 8.0, ((0, 8),), (0, 1, 8, 2.0), jnp.float32),
        "weight_up": centred(arg_keys[7], (WIDTH, INNER), WIDTH ** -0.5, 0.1875, ((0, 8), (1, 4)), jnp.float32),
        "weight_down": centred(arg_keys[8], (INNER, WIDTH), INNER ** -0.5, 0.09375, ((0, 4), (1, 8)), jnp.float32),
        "weight_query": centred(arg_keys[9], (WIDTH, ATTN), WIDTH ** -0.5, 0.1875, ((0, 8), (1, 4)), jnp.float32),
        "weight_key": centred(arg_keys[10], (WIDTH, ATTN), WIDTH ** -0.5, 0.1875, ((0, 8), (1, 4)), jnp.float32),
        "weight_value": centred(arg_keys[11], (WIDTH, ATTN), WIDTH ** -0.5, 0.1875, ((0, 8), (1, 4)), jnp.float32),
        "weight_mixed": centred(arg_keys[12], (ATTN, WIDTH), ATTN ** -0.5, 0.1875, ((0, 4), (1, 8)), jnp.float32),
        "weight_norm": jnp.clip(1.0 + 0.15 * jax.random.normal(arg_keys[13], (WIDTH,), jnp.float32), 0.25, 1.75),
        "moment_up": centred(arg_keys[14], (WIDTH, INNER), 0.3, 1.75, ((0, 8), (1, 4)), jnp.float32),
        "moment_down": centred(arg_keys[15], (INNER, WIDTH), 0.3, 1.75, ((0, 4), (1, 8)), jnp.float32),
        "moment_query": centred(arg_keys[16], (WIDTH, ATTN), 0.3, 1.75, ((0, 8), (1, 4)), jnp.float32),
        "moment_key": centred(arg_keys[17], (WIDTH, ATTN), 0.3, 1.75, ((0, 8), (1, 4)), jnp.float32),
        "moment_value": centred(arg_keys[18], (WIDTH, ATTN), 0.3, 1.75, ((0, 8), (1, 4)), jnp.float32),
        "moment_mixed": centred(arg_keys[19], (ATTN, WIDTH), 0.3, 1.75, ((0, 4), (1, 8)), jnp.float32),
        "moment_norm": centred(arg_keys[20], (WIDTH,), 0.3, 1.75, ((0, 8),), jnp.float32),
    }


learn_rate = 0.1
hold_rate = 0.7


def reference(grad_up, grad_down, grad_query, grad_key, grad_value, grad_mixed, grad_norm, weight_up, weight_down, weight_query, weight_key, weight_value, weight_mixed, weight_norm, moment_up, moment_down, moment_query, moment_key, moment_value, moment_mixed, moment_norm):
    mean_up = jnp.sum(grad_up.astype(jnp.float32), axis=0) * REPLICAS ** -0.5
    mean_down = jnp.sum(grad_down.astype(jnp.float32), axis=0) * REPLICAS ** -0.5
    mean_query = jnp.sum(grad_query.astype(jnp.float32), axis=0) * REPLICAS ** -0.5
    mean_key = jnp.sum(grad_key.astype(jnp.float32), axis=0) * REPLICAS ** -0.5
    mean_value = jnp.sum(grad_value.astype(jnp.float32), axis=0) * REPLICAS ** -0.5
    mean_mixed = jnp.sum(grad_mixed.astype(jnp.float32), axis=0) * REPLICAS ** -0.5
    mean_norm = jnp.sum(grad_norm.astype(jnp.float32), axis=0) * REPLICAS ** -0.5
    state_new_up = hold_rate * moment_up + mean_up
    new_up = weight_up - learn_rate * state_new_up
    state_new_down = hold_rate * moment_down + mean_down
    new_down = weight_down - learn_rate * state_new_down
    state_new_query = hold_rate * moment_query + mean_query
    new_query = weight_query - learn_rate * state_new_query
    state_new_key = hold_rate * moment_key + mean_key
    new_key = weight_key - learn_rate * state_new_key
    state_new_value = hold_rate * moment_value + mean_value
    new_value = weight_value - learn_rate * state_new_value
    state_new_mixed = hold_rate * moment_mixed + mean_mixed
    new_mixed = weight_mixed - learn_rate * state_new_mixed
    state_new_norm = hold_rate * moment_norm + mean_norm
    new_norm = weight_norm - learn_rate * state_new_norm
    copy_up = new_up.astype(jnp.bfloat16)
    copy_down = new_down.astype(jnp.bfloat16)
    copy_query = new_query.astype(jnp.bfloat16)
    copy_key = new_key.astype(jnp.bfloat16)
    copy_value = new_value.astype(jnp.bfloat16)
    copy_mixed = new_mixed.astype(jnp.bfloat16)
    copy_norm = new_norm.astype(jnp.bfloat16)
    return copy_up, copy_down, copy_query, copy_key, copy_value, copy_mixed, copy_norm, new_up, new_down, new_query, new_key, new_value, new_mixed, new_norm, state_new_up, state_new_down, state_new_query, state_new_key, state_new_value, state_new_mixed, state_new_norm
```

```python
import functools

import jax
import jax.numpy as jnp
from jax import lax
from jax.experimental import pallas as pl
from jax.experimental.pallas import tpu as pltpu
from jax.sharding import PartitionSpec as P

learn_rate = 0.1
hold_rate = 0.7
AXIS = "batch"
LANES = 128
PAD = 8


names = ("up", "down", "query", "key", "value", "mixed", "norm")
cut_dim = {"up": 0, "down": 1, "query": 0, "key": 0, "value": 0, "mixed": 1}


class Plan:
    def __init__(self, steps, dim, members, shards, norm):
        self.steps, self.dim, self.members, self.norm = steps, dim, members, norm
        self.shards = shards
        self.offsets, total = [], 0
        for name in members:
            self.offsets.append(total)
            total += shards[name][1 - dim]
        first = shards[members[0]]
        total += PAD if norm else 0
        self.block = (first[0], total) if dim == 0 else (total, first[1])

    def part(self, t):
        rows, columns = self.shards[self.members[t]]
        start = self.offsets[t]
        if self.dim == 0:
            return (slice(None), slice(start, start + columns))
        return (slice(start, start + rows), slice(None))

    def pad(self):
        return (slice(self.block[0] - PAD, self.block[0]), slice(None))


def mask_of(code, me, steps):
    colour = (me & 1) ^ (code & 1)
    mask = code & 1
    for k in range(1, steps):
        mask = mask + ((code >> k) & 1) * ((1 << k) + colour * ((1 << (steps - k)) - (1 << k)))
    return mask


def owner_of(code, steps):
    me = lax.axis_index(AXIS)
    return me ^ mask_of(code, me, steps)


def partners(k, steps):
    pairs = []
    for me in range(1 << steps):
        if k == 0:
            bit = 0
        else:
            bit = k if me & 1 == 0 else steps - k
        pairs.append((me, me ^ (1 << bit)))
    return pairs


def exchange(x, k, steps):
    return lax.ppermute(x, AXIS, partners(k, steps))


def split_rows(x):
    high = x.astype(jnp.bfloat16).astype(jnp.float32)
    low = x - high
    row = lax.broadcasted_iota(jnp.int32, (PAD, x.shape[1]), 0)
    return jnp.where(row == 0, high, jnp.where(row == 1, low, 0.0)).astype(jnp.bfloat16)


def grad_specs(plan, code):
    specs = []
    for name in plan.members:
        shape = plan.shards[name]
        if plan.dim == 0:
            specs.append(pl.BlockSpec(shape, lambda q: (owner_of(code(q), plan.steps), 0)))
        else:
            specs.append(pl.BlockSpec(shape, lambda q: (0, owner_of(code(q), plan.steps))))
    if plan.norm:
        size = plan.shards["norm"]
        specs.append(pl.BlockSpec((1, size), lambda q: (0, owner_of(code(q), plan.steps))))
    return specs


def gathered(plan, t, grads, received):
    part = plan.part(t)
    total = grads[t][...]
    for r in received:
        total += r[(0,) + part].astype(jnp.float32)
    return total


def gathered_norm(plan, grads, received):
    total = grads[-1][...]
    for r in received:
        total += jnp.sum(r[(0,) + plan.pad()].astype(jnp.float32), axis=0, keepdims=True)
    return total


def send_kernel(plan, k, *refs):
    n = len(plan.members) + int(plan.norm)
    grads, received, out = refs[:n], refs[n : n + k], refs[n + k]
    for t in range(len(plan.members)):
        out[(0,) + plan.part(t)] = gathered(plan, t, grads, received).astype(jnp.bfloat16)
    if plan.norm:
        out[(0,) + plan.pad()] = split_rows(gathered_norm(plan, grads, received))


def send_stage(plan, k, grads, received):
    count = 1 << (plan.steps - 1 - k)

    def code(q):
        return (q << (k + 1)) + (1 << k)

    block = (1,) + plan.block
    specs = grad_specs(plan, code)
    for l in range(k):
        specs.append(pl.BlockSpec(block, lambda q, l=l: (code(q) >> (l + 1), 0, 0)))
    size = count * plan.block[0] * plan.block[1]
    return pl.pallas_call(
        functools.partial(send_kernel, plan, k),
        grid=(count,),
        out_shape=jax.ShapeDtypeStruct((count,) + plan.block, jnp.bfloat16),
        in_specs=specs,
        out_specs=pl.BlockSpec(block, lambda q: (q, 0, 0)),
        cost_estimate=pl.CostEstimate(flops=4 * size, bytes_accessed=(6 + 2 * k) * size, transcendentals=0),
        compiler_params=pltpu.CompilerParams(vmem_limit_bytes=16 * 2**20),
        name=f"send{k}_{plan.members[0]}",
    )(*grads, *received)


def update_kernel(plan, rate, *refs):
    m = len(plan.members)
    n = m + int(plan.norm)
    grads, refs = refs[:n], refs[n:]
    received, refs = refs[: plan.steps], refs[plan.steps :]
    weights, moments, copy, new, state = refs[:n], refs[n : 2 * n], refs[2 * n], refs[2 * n + 1 : 3 * n + 1], refs[3 * n + 1 :]
    for t in range(n):
        if t < m:
            mean = gathered(plan, t, grads, received) * rate
        else:
            mean = gathered_norm(plan, grads, received) * rate
        held = hold_rate * moments[t][...] + mean
        fresh = weights[t][...] - learn_rate * held
        state[t][...] = held
        new[t][...] = fresh
        if t < m:
            copy[(0,) + plan.part(t)] = fresh.astype(jnp.bfloat16)
        else:
            copy[(0,) + plan.pad()] = split_rows(fresh)


def update_stage(plan, grads, received, weights, moments):
    block = (1,) + plan.block
    specs = grad_specs(plan, lambda q: 0 * q)
    specs += [pl.BlockSpec(block, lambda q: (0, 0, 0)) for _ in received]
    shards = [plan.shards[name] for name in plan.members]
    if plan.norm:
        shards.append((1, plan.shards["norm"]))
    whole = [pl.BlockSpec(shape, lambda q: (0, 0)) for shape in shards]
    arrays = [jax.ShapeDtypeStruct(shape, jnp.float32) for shape in shards]
    size = plan.block[0] * plan.block[1]
    n = len(shards)
    out = pl.pallas_call(
        functools.partial(update_kernel, plan, (1 << plan.steps) ** (-0.5)),
        grid=(1,),
        out_shape=[jax.ShapeDtypeStruct(block, jnp.bfloat16)] + arrays + arrays,
        in_specs=specs + whole + whole,
        out_specs=[pl.BlockSpec(block, lambda q: (0, 0, 0))] + whole + whole,
        cost_estimate=pl.CostEstimate(flops=12 * size, bytes_accessed=28 * size, transcendentals=0),
        compiler_params=pltpu.CompilerParams(vmem_limit_bytes=24 * 2**20),
        name=f"update_{plan.members[0]}",
    )(*grads, *received, *weights, *moments)
    return out[0], out[1 : 1 + n], out[1 + n :]


def collect_kernel(plan, codes, *refs):
    count = len(codes)
    m = len(plan.members)
    pieces, refs = refs[:count], refs[count:]
    outs, refs = refs[:m], refs[m:]
    if plan.norm:
        norm_out, refs = refs[0], refs[1:]
    slots, in_sems, out_sems = refs[:3]
    reads = []
    for p in range(count):
        reads.append(pltpu.make_async_copy(pieces[p].at[0], slots.at[p], in_sems.at[p]))
        reads[-1].start()
    writes = []
    for p in range(count):
        reads[p].wait()
        owner = owner_of(codes[p], plan.steps)
        for t in range(m):
            rows, columns = plan.shards[plan.members[t]]
            if plan.dim == 0:
                place = (pl.ds(pl.multiple_of(owner * rows, rows), rows), slice(None))
            else:
                place = (slice(None), pl.ds(pl.multiple_of(owner * columns, columns), columns))
            writes.append(pltpu.make_async_copy(slots.at[(p,) + plan.part(t)], outs[t].at[place], out_sems.at[p, t]))
            writes[-1].start()
        if plan.norm:
            row = jnp.sum(slots[(p,) + plan.pad()].astype(jnp.float32), axis=0, keepdims=True)
            norm_out[pl.ds(owner, 1), :] = row
    for w in writes:
        w.wait()


def collect_stage(plan, pieces):
    codes = tuple(code for code, _ in pieces)
    count = len(codes)
    m = len(plan.members)
    shapes = []
    for name in plan.members:
        rows, columns = plan.shards[name]
        shapes.append((rows * count, columns) if plan.dim == 0 else (rows, columns * count))
    out_shape = [jax.ShapeDtypeStruct(shape, jnp.bfloat16) for shape in shapes]
    out_specs = [pl.BlockSpec(memory_space=pl.ANY)] * m
    if plan.norm:
        out_shape.append(jax.ShapeDtypeStruct((count, plan.shards["norm"]), jnp.float32))
        out_specs.append(pl.BlockSpec(memory_space=pltpu.VMEM))
    size = count * plan.block[0] * plan.block[1]
    return pl.pallas_call(
        functools.partial(collect_kernel, plan, codes),
        out_shape=out_shape,
        in_specs=[pl.BlockSpec(memory_space=pl.ANY)] * count,
        out_specs=out_specs,
        scratch_shapes=[
            pltpu.VMEM((count,) + plan.block, jnp.bfloat16),
            pltpu.SemaphoreType.DMA((count,)),
            pltpu.SemaphoreType.DMA((count, m)),
        ],
        cost_estimate=pl.CostEstimate(flops=4 * size, bytes_accessed=4 * size, transcendentals=0),
        compiler_params=pltpu.CompilerParams(vmem_limit_bytes=16 * 2**20),
        name=f"collect_{plan.members[0]}",
    )(*[piece for _, piece in pieces])


def fast_body(*args):
    grads = dict(zip(names, args[:7]))
    weights = dict(zip(names, args[7:14]))
    moments = dict(zip(names, args[14:21]))
    size = lax.axis_size(AXIS)
    steps = size.bit_length() - 1
    shards = {name: weights[name].shape for name in names[:-1]}
    shards["norm"] = weights["norm"].shape[0]
    plans = (
        Plan(steps, 1, ("down", "mixed"), shards, True),
        Plan(steps, 0, ("up", "query", "key", "value"), shards, False),
    )

    def inputs(plan, arrays, squeeze):
        out = [arrays[name][0] if squeeze else arrays[name] for name in plan.members]
        if plan.norm:
            out.append(arrays["norm"] if squeeze else arrays["norm"].reshape(1, -1))
        return out

    g = [inputs(plan, grads, True) for plan in plans]
    received = [[] for _ in plans]
    for k in range(steps):
        for c, plan in enumerate(plans):
            sent = send_stage(plan, k, g[c], received[c])
            received[c].append(exchange(sent, k, steps))
    copies, news, states = {}, {}, {}
    pieces = []
    for c, plan in enumerate(plans):
        copy, new, state = update_stage(
            plan, g[c], received[c], inputs(plan, weights, False), inputs(plan, moments, False)
        )
        members = plan.members + (("norm",) if plan.norm else ())
        for name, a, b in zip(members, new, state):
            news[name] = a.reshape(weights[name].shape)
            states[name] = b.reshape(weights[name].shape)
        pieces.append([(0, copy)])
    for k in reversed(range(steps)):
        for c in range(len(plans)):
            pieces[c] += [(code | 1 << k, exchange(x, k, steps)) for code, x in pieces[c]]
    for c, plan in enumerate(plans):
        out = collect_stage(plan, pieces[c])
        for t, name in enumerate(plan.members):
            copies[name] = out[t]
        if plan.norm:
            copies["norm"] = out[-1].reshape(-1).astype(jnp.bfloat16)
    return tuple(table[name] for table in (copies, news, states) for name in names)


def fits(args):
    size = lax.axis_size(AXIS)
    good = size >= 4 and size & (size - 1) == 0
    for name, weight in zip(names, args[7:14]):
        good = good and weight.shape[-1] % LANES == 0
        if weight.ndim == 2:
            good = good and weight.shape[0] % 16 == 0
            if cut_dim[name] == 1:
                good = good and weight.shape[1] == LANES
        else:
            good = good and weight.shape[0] == LANES
    return good


def body(*args):
    return fast_body(*args) if fits(args) else plain_body(*args)


def plain_body(
    grad_up,
    grad_down,
    grad_query,
    grad_key,
    grad_value,
    grad_mixed,
    grad_norm,
    weight_up,
    weight_down,
    weight_query,
    weight_key,
    weight_value,
    weight_mixed,
    weight_norm,
    moment_up,
    moment_down,
    moment_query,
    moment_key,
    moment_value,
    moment_mixed,
    moment_norm,
):
    mean_up, mean_down, mean_query, mean_key, mean_value, mean_mixed = (
        lax.psum_scatter(
            grad_up[0].astype(jnp.bfloat16), "batch", scatter_dimension=0, tiled=True
        ).astype(jnp.float32),
        lax.psum_scatter(
            grad_down[0].astype(jnp.bfloat16), "batch", scatter_dimension=1, tiled=True
        ).astype(jnp.float32),
        lax.psum_scatter(
            grad_query[0].astype(jnp.bfloat16), "batch", scatter_dimension=0, tiled=True
        ).astype(jnp.float32),
        lax.psum_scatter(
            grad_key[0].astype(jnp.bfloat16), "batch", scatter_dimension=0, tiled=True
        ).astype(jnp.float32),
        lax.psum_scatter(
            grad_value[0].astype(jnp.bfloat16), "batch", scatter_dimension=0, tiled=True
        ).astype(jnp.float32),
        lax.psum_scatter(
            grad_mixed[0].astype(jnp.bfloat16), "batch", scatter_dimension=1, tiled=True
        ).astype(jnp.float32),
    )
    whole_norm = lax.psum(grad_norm[0], "batch")
    place = lax.axis_index("batch")
    mean_norm = lax.dynamic_slice_in_dim(
        whole_norm, place * weight_norm.shape[0], weight_norm.shape[0]
    )
    mean_rate = lax.axis_size("batch") ** (-0.5)
    mean_up = mean_up * mean_rate
    mean_down = mean_down * mean_rate
    mean_query = mean_query * mean_rate
    mean_key = mean_key * mean_rate
    mean_value = mean_value * mean_rate
    mean_mixed = mean_mixed * mean_rate
    mean_norm = mean_norm * mean_rate
    state_new_up = hold_rate * moment_up + mean_up
    new_up = weight_up - learn_rate * state_new_up
    state_new_down = hold_rate * moment_down + mean_down
    new_down = weight_down - learn_rate * state_new_down
    state_new_query = hold_rate * moment_query + mean_query
    new_query = weight_query - learn_rate * state_new_query
    state_new_key = hold_rate * moment_key + mean_key
    new_key = weight_key - learn_rate * state_new_key
    state_new_value = hold_rate * moment_value + mean_value
    new_value = weight_value - learn_rate * state_new_value
    state_new_mixed = hold_rate * moment_mixed + mean_mixed
    new_mixed = weight_mixed - learn_rate * state_new_mixed
    state_new_norm = hold_rate * moment_norm + mean_norm
    new_norm = weight_norm - learn_rate * state_new_norm
    copy_up, copy_down, copy_query, copy_key, copy_value, copy_mixed, copy_norm = (
        lax.all_gather(new_up.astype(jnp.bfloat16), "batch", axis=0, tiled=True),
        lax.all_gather(new_down.astype(jnp.bfloat16), "batch", axis=1, tiled=True),
        lax.all_gather(new_query.astype(jnp.bfloat16), "batch", axis=0, tiled=True),
        lax.all_gather(new_key.astype(jnp.bfloat16), "batch", axis=0, tiled=True),
        lax.all_gather(new_value.astype(jnp.bfloat16), "batch", axis=0, tiled=True),
        lax.all_gather(new_mixed.astype(jnp.bfloat16), "batch", axis=1, tiled=True),
        lax.all_gather(new_norm.astype(jnp.bfloat16), "batch", axis=0, tiled=True),
    )
    return (
        copy_up,
        copy_down,
        copy_query,
        copy_key,
        copy_value,
        copy_mixed,
        copy_norm,
        new_up,
        new_down,
        new_query,
        new_key,
        new_value,
        new_mixed,
        new_norm,
        state_new_up,
        state_new_down,
        state_new_query,
        state_new_key,
        state_new_value,
        state_new_mixed,
        state_new_norm,
    )


def solution(mesh):
    in_specs = (
        P("batch", None, "cols"),
        P("batch", "cols", None),
        P("batch", None, "cols"),
        P("batch", None, "cols"),
        P("batch", None, "cols"),
        P("batch", "cols", None),
        P("batch", None),
        P("batch", "cols"),
        P("cols", "batch"),
        P("batch", "cols"),
        P("batch", "cols"),
        P("batch", "cols"),
        P("cols", "batch"),
        P("batch"),
        P("batch", "cols"),
        P("cols", "batch"),
        P("batch", "cols"),
        P("batch", "cols"),
        P("batch", "cols"),
        P("cols", "batch"),
        P("batch"),
    )
    out_specs = (
        P(None, "cols"),
        P("cols", None),
        P(None, "cols"),
        P(None, "cols"),
        P(None, "cols"),
        P("cols", None),
        P(),
        P("batch", "cols"),
        P("cols", "batch"),
        P("batch", "cols"),
        P("batch", "cols"),
        P("batch", "cols"),
        P("cols", "batch"),
        P("batch"),
        P("batch", "cols"),
        P("cols", "batch"),
        P("batch", "cols"),
        P("batch", "cols"),
        P("batch", "cols"),
        P("cols", "batch"),
        P("batch"),
    )
    return jax.shard_map(body, mesh=mesh, in_specs=in_specs, out_specs=out_specs, check_vma=False)
```

```python
import functools

import jax
import jax.numpy as jnp
from jax import lax
from jax.experimental import pallas as pl
from jax.experimental.pallas import tpu as pltpu
from jax.sharding import PartitionSpec as P


learn_rate = 0.1
hold_rate = 0.7
AXIS, COLS = "batch", "cols"
LANES = 128
PAD = 8


names = ("up", "down", "query", "key", "value", "mixed", "norm")
cut_dim = {"up": 0, "down": 1, "query": 0, "key": 0, "value": 0, "mixed": 1}


class Plan:
    def __init__(self, steps, dim, members, shards, norm):
        self.steps, self.dim, self.members, self.norm = steps, dim, members, norm
        self.shards = shards
        self.offsets, total = [], 0
        for name in members:
            self.offsets.append(total)
            total += shards[name][1 - dim]
        first = shards[members[0]]
        total += PAD if norm else 0
        self.block = (first[0], total) if dim == 0 else (total, first[1])
        self.groups = [self]

    def part(self, t):
        rows, columns = self.shards[self.members[t]]
        start = self.offsets[t]
        if self.dim == 0:
            return (slice(None), slice(start, start + columns))
        return (slice(start, start + rows), slice(None))

    def place(self, t, owner):
        rows, columns = self.shards[self.members[t]]
        if self.dim == 0:
            return (pl.ds(pl.multiple_of(owner * rows, rows), rows), slice(None))
        return (slice(None), pl.ds(pl.multiple_of(owner * columns, columns), columns))

    def pad_row(self):
        return slice(self.block[0] - PAD, self.block[0] - PAD + 1)

    def pad(self):
        return (slice(self.block[0] - PAD, self.block[0]), slice(None))


def mask_of(code, me, steps):
    colour = (me & 1) ^ (code & 1)
    mask = code & 1
    for k in range(1, steps):
        mask = mask + ((code >> k) & 1) * ((1 << k) + colour * ((1 << (steps - k)) - (1 << k)))
    return mask


def owner_of(code, steps):
    me = lax.axis_index(AXIS)
    return me ^ mask_of(code, me, steps)


def partners(k, steps):
    pairs = []
    for me in range(1 << steps):
        if k == 0:
            bit = 0
        else:
            bit = k if me & 1 == 0 else steps - k
        pairs.append((me, me ^ (1 << bit)))
    return pairs


def exchange(x, k, steps):
    return lax.ppermute(x, AXIS, partners(k, steps))


def split_rows(x):
    high = x.astype(jnp.bfloat16).astype(jnp.float32)
    low = x - high
    row = lax.broadcasted_iota(jnp.int32, (PAD, x.shape[1]), 0)
    return jnp.where(row == 0, high, jnp.where(row == 1, low, 0.0)).astype(jnp.bfloat16)


def gathered(plan, t, own, received):
    part = (0,) + plan.part(t)
    total = own[part]
    for r in received:
        total += r[part].astype(jnp.float32)
    return total


def gathered_norm(plan, own, received):
    total = own[0, plan.pad_row(), :]
    for r in received:
        total += jnp.sum(r[(0,) + plan.pad()].astype(jnp.float32), axis=0, keepdims=True)
    return total


def send_kernel(plan, own, *refs):
    received, out = refs[:-1], refs[-1]
    for t in range(len(plan.members)):
        out[(0,) + plan.part(t)] = gathered(plan, t, own, received).astype(jnp.bfloat16)
    if plan.norm:
        out[(0,) + plan.pad()] = split_rows(gathered_norm(plan, own, received))


def first_kernel(jobs, *refs):
    inputs = []
    for plan, _, _ in jobs:
        n = len(plan.members) + int(plan.norm)
        inputs.append(refs[:n])
        refs = refs[n:]
    outs, scratches, sems = refs[: len(jobs)], refs[len(jobs) : -1], refs[-1]
    count = 0

    def fetch(plan, grads, code, target):
        nonlocal count
        owner = owner_of(code, plan.steps)
        pairs = [(grads[t].at[plan.place(t, owner)], plan.part(t)) for t in range(len(plan.members))]
        if plan.norm:
            pairs.append((grads[-1].at[:, pl.ds(pl.multiple_of(owner * LANES, LANES), LANES)], (plan.pad_row(), slice(None))))
        copies = []
        for source, part in pairs:
            copies.append(pltpu.make_async_copy(source, target.at[part], sems.at[count]))
            copies[-1].start()
            count += 1
        return copies

    landing, reads = [], []
    for (plan, codes, keep), grads, out in zip(jobs, inputs, outs):
        if keep:
            landing.append(out)
        else:
            landing.append(scratches[0])
            scratches = scratches[1:]
        reads.append([fetch(plan, grads, code, landing[-1].at[q]) for q, code in enumerate(codes)])
    for (plan, codes, keep), out, source, copies in zip(jobs, outs, landing, reads):
        for q in range(len(codes)):
            for t, copy in enumerate(copies[q]):
                copy.wait()
                if keep:
                    continue
                if t < len(plan.members):
                    out[(q,) + plan.part(t)] = source[(q,) + plan.part(t)].astype(jnp.bfloat16)
                else:
                    out[(q,) + plan.pad()] = split_rows(source[q, plan.pad_row(), :])


def first_stage(jobs):
    listed, operands, out_shape, scratch = [], [], [], []
    copies = size = 0
    for plan, (base, stride, count), grads, keep in jobs:
        shape = (count,) + plan.block
        listed.append((plan, [base + (q << stride) - int(keep) for q in range(count)], keep))
        operands += [pltpu.with_memory_space_constraint(g, pltpu.HBM) for g in grads]
        out_shape.append(jax.ShapeDtypeStruct(shape, jnp.float32 if keep else jnp.bfloat16))
        if not keep:
            scratch.append(pltpu.VMEM(shape, jnp.float32))
        copies += count * len(grads)
        size += shape[0] * shape[1] * shape[2]
    return pl.pallas_call(
        functools.partial(first_kernel, listed),
        out_shape=out_shape,
        in_specs=[pl.BlockSpec(memory_space=pl.ANY)] * len(operands),
        out_specs=[pl.BlockSpec(memory_space=pltpu.VMEM)] * len(out_shape),
        scratch_shapes=scratch + [pltpu.SemaphoreType.DMA((copies,))],
        cost_estimate=pl.CostEstimate(flops=4 * size, bytes_accessed=6 * size, transcendentals=0),
        compiler_params=pltpu.CompilerParams(vmem_limit_bytes=16 * 2**20),
    )(*operands)


def messages_of(k, steps):
    if k == steps - 1:
        return [(1 << k, k + 1, 1)]
    high = (3 << k, k + 2, 1 << (steps - 2 - k))
    low = (1 << k, k + 2, 1 << (steps - 2 - k))
    if k > 0 or steps < 3:
        return [high, low]
    half = high[2] // 2
    return [(7 << k, k + 3, half), (3 << k, k + 3, half), low]


def find(message, k, kept, received):
    base, stride, count = message
    codes = [base + (q << stride) for q in range(count)]
    places = []
    for table in [kept] + received[:k]:
        for (first, step, size), array in table:
            held = [first + (i << step) for i in range(size)]
            if all(code in held for code in codes):
                places.append((array, first, step))
                break
    return places


def send_stage(plan, k, message, kept, received):
    base, stride, count = message
    block = (1,) + plan.block
    parts, specs = [], []
    for array, first, step in find(message, k, kept, received):
        parts.append(array)
        specs.append(pl.BlockSpec(block, lambda q, first=first, step=step: ((base + (q << stride) - first) >> step, 0, 0)))
    size = count * plan.block[0] * plan.block[1]
    return pl.pallas_call(
        functools.partial(send_kernel, plan),
        grid=(count,),
        out_shape=jax.ShapeDtypeStruct((count,) + plan.block, jnp.bfloat16),
        in_specs=specs,
        out_specs=pl.BlockSpec(block, lambda q: (q, 0, 0)),
        cost_estimate=pl.CostEstimate(flops=4 * size, bytes_accessed=(6 + 2 * k) * size, transcendentals=0),
        compiler_params=pltpu.CompilerParams(vmem_limit_bytes=16 * 2**20),
    )(*parts)


def update_kernel(plan, rate, *refs):
    m = len(plan.members)
    n = m + int(plan.norm)
    own, received, refs = refs[0], refs[1 : 1 + plan.steps], refs[1 + plan.steps :]
    weights, moments, refs = refs[:n], refs[n : 2 * n], refs[2 * n :]
    copies, refs = refs[: len(plan.groups)], refs[len(plan.groups) :]
    new, state = refs[:n], refs[n:]
    for t in range(n):
        if t < m:
            mean = gathered(plan, t, own, received) * rate
        else:
            mean = gathered_norm(plan, own, received) * rate
        held = hold_rate * moments[t][...] + mean
        fresh = weights[t][...] - learn_rate * held
        state[t][...] = held
        new[t][...] = fresh
        for group, copy in zip(plan.groups, copies):
            if t == m:
                if group.norm:
                    copy[(0,) + group.pad()] = split_rows(fresh)
            elif plan.members[t] in group.members:
                place = group.part(group.members.index(plan.members[t]))
                copy[(0,) + place] = fresh.astype(jnp.bfloat16)


def update_stage(plan, kept, received, weights, moments):
    block = (1,) + plan.block
    parts = [array for array, _, _ in find((0, 0, 1), plan.steps, kept, received)]
    specs = [pl.BlockSpec(block, lambda q: (0, 0, 0)) for _ in parts]
    shards = [plan.shards[name] for name in plan.members]
    if plan.norm:
        shards.append((1, plan.shards["norm"]))
    whole = [pl.BlockSpec(shape, lambda q: (0, 0)) for shape in shards]
    arrays = [jax.ShapeDtypeStruct(shape, jnp.float32) for shape in shards]
    copies = [(1,) + group.block for group in plan.groups]
    size = plan.block[0] * plan.block[1]
    n, m = len(shards), len(copies)
    out = pl.pallas_call(
        functools.partial(update_kernel, plan, (1 << plan.steps) ** (-0.5)),
        grid=(1,),
        out_shape=[jax.ShapeDtypeStruct(shape, jnp.bfloat16) for shape in copies] + arrays + arrays,
        in_specs=specs + whole + whole,
        out_specs=[pl.BlockSpec(shape, lambda q: (0, 0, 0)) for shape in copies] + whole + whole,
        cost_estimate=pl.CostEstimate(flops=12 * size, bytes_accessed=28 * size, transcendentals=0),
        compiler_params=pltpu.CompilerParams(vmem_limit_bytes=24 * 2**20),
    )(*parts, *weights, *moments)
    return out[:m], out[m : m + n], out[m + n :]


def collect_kernel(jobs, aliased, *refs):
    inputs = sum(len(codes) for _, codes, _ in jobs)
    pieces, refs = refs[:inputs], refs[inputs + aliased :]
    writes, norms = [], []
    outs, count = refs, 0
    for plan, _, _ in jobs:
        count += len(plan.members) + int(plan.norm)
    outs, scratch = refs[:count], refs[count:]
    sems = scratch[0]
    for plan, codes, fresh in jobs:
        m = len(plan.members)
        held, pieces = dict(zip(codes, pieces)), pieces[len(codes) :]
        targets, outs = outs[: m + int(plan.norm)], outs[m + int(plan.norm) :]
        if plan.norm:
            rows, row_sems, table = scratch[1:]
            reads = []
            for p, code in enumerate(codes):
                reads.append(pltpu.make_async_copy(held[code].at[(0,) + plan.pad()], rows.at[p], row_sems.at[p]))
                reads[-1].start()
            norms.append((plan, codes, reads, targets[-1]))
        for code in fresh:
            owner = owner_of(code, plan.steps)
            for t in range(m):
                place = plan.place(t, owner)
                source = held[code].at[(0,) + plan.part(t)]
                writes.append(pltpu.make_async_copy(source, targets[t].at[place], sems.at[len(writes)]))
                writes[-1].start()
    for plan, codes, reads, target in norms:
        for p, code in enumerate(codes):
            reads[p].wait()
            row = jnp.sum(rows[p].astype(jnp.float32), axis=0, keepdims=True)
            table[pl.ds(owner_of(code, plan.steps), 1), :] = row
        target[...] = table[...].astype(jnp.bfloat16)
    for w in writes:
        w.wait()


def collect_stage(jobs):
    operands, filled, out_shape, out_specs, aliases = [], [], [], [], {}
    scratch, copies, moved = [], 0, 0
    inputs = sum(len(pieces) for _, pieces, _, _ in jobs)
    for plan, pieces, fresh, rest in jobs:
        operands += list(pieces.values())
        copies += len(fresh) * len(plan.members)
        moved += len(fresh) * plan.block[0] * plan.block[1]
        size = 1 << plan.steps
        for t, name in enumerate(plan.members):
            rows, columns = plan.shards[name]
            if rest is not None:
                aliases[inputs + len(filled)] = len(out_shape)
                filled.append(rest[t])
            shape = (rows * size, columns) if plan.dim == 0 else (rows, columns * size)
            out_shape.append(jax.ShapeDtypeStruct(shape, jnp.bfloat16))
            out_specs.append(pl.BlockSpec(memory_space=pltpu.HBM))
        if plan.norm:
            width = plan.shards["norm"]
            out_shape.append(jax.ShapeDtypeStruct((size, width), jnp.bfloat16))
            out_specs.append(pl.BlockSpec(memory_space=pltpu.VMEM))
            scratch = [
                pltpu.VMEM((len(pieces), PAD, width), jnp.bfloat16),
                pltpu.SemaphoreType.DMA((len(pieces),)),
                pltpu.VMEM((size, width), jnp.float32),
            ]
    listed = tuple((plan, tuple(pieces), tuple(fresh)) for plan, pieces, fresh, _ in jobs)
    return pl.pallas_call(
        functools.partial(collect_kernel, listed, len(filled)),
        out_shape=out_shape,
        in_specs=[pl.BlockSpec(memory_space=pl.ANY)] * (inputs + len(filled)),
        out_specs=out_specs,
        scratch_shapes=[pltpu.SemaphoreType.DMA((copies,))] + scratch,
        input_output_aliases=aliases,
        cost_estimate=pl.CostEstimate(flops=4 * moved, bytes_accessed=4 * moved, transcendentals=0),
        compiler_params=pltpu.CompilerParams(vmem_limit_bytes=4 * 2**20),
    )(*operands, *filled)


def fast_body(*args):
    grads = dict(zip(names, args[:7]))
    weights = dict(zip(names, args[7:14]))
    moments = dict(zip(names, args[14:21]))
    size = lax.axis_size(AXIS)
    steps = size.bit_length() - 1
    shards = {name: weights[name].shape for name in names[:-1]}
    shards["norm"] = weights["norm"].shape[0]
    plans = (
        Plan(steps, 1, ("down", "mixed"), shards, True),
        Plan(steps, 0, ("up", "query", "key", "value"), shards, False),
    )
    plans[0].groups = [Plan(steps, 1, ("down",), shards, True), Plan(steps, 1, ("mixed",), shards, False)]

    def inputs(plan, arrays, squeeze):
        out = [arrays[name][0] if squeeze else arrays[name] for name in plan.members]
        if plan.norm:
            out.append(arrays["norm"] if squeeze else arrays["norm"].reshape(1, -1))
        return out

    g = [inputs(plan, grads, True) for plan in plans]
    received = [[[] for _ in range(steps)] for _ in plans]
    kept = [[] for _ in plans]
    stage = messages_of(0, steps)
    for i, message in enumerate(stage):
        for c, plan in enumerate(plans):
            own = [(c, message)]
            if i == 0:
                own = [] if c == 0 else [(0, message)]
            elif i == 1:
                own = [(1, stage[0])] if c == 0 else [(0, message), (1, message)]
            jobs = [(plan, message, g[c], False)] + [(plans[d], which, g[d], True) for d, which in own]
            sent, *rest = first_stage(jobs)
            for (d, (base, stride, count)), array in zip(own, rest):
                kept[d].append(((base - 1, stride, count), array))
            received[c][0].append(((message[0] - 1,) + message[1:], exchange(sent, 0, steps)))
    for k in range(1, steps):
        for message in messages_of(k, steps):
            for c, plan in enumerate(plans):
                sent = send_stage(plan, k, message, kept[c], received[c])
                received[c][k].append(((message[0] - (1 << k),) + message[1:], exchange(sent, k, steps)))
    copies, news, states = {}, {}, {}
    groups, pieces = [], []
    for c, plan in enumerate(plans):
        fresh, new, state = update_stage(
            plan, kept[c], received[c], inputs(plan, weights, False), inputs(plan, moments, False)
        )
        members = plan.members + (("norm",) if plan.norm else ())
        for name, a, b in zip(members, new, state):
            news[name] = a.reshape(weights[name].shape)
            states[name] = b.reshape(weights[name].shape)
        groups += plan.groups
        pieces += [{0: x} for x in fresh]
    for k in reversed(range(steps)):
        for held in pieces:
            for code, x in list(held.items()):
                held[code | 1 << k] = exchange(x, k, steps)
    down, mixed, rows = range(3)
    m = len(groups[rows].members)

    def only(i, codes):
        return {code: pieces[i][code] for code in codes}

    out = collect_stage([(groups[down], pieces[down], range(size), None)])
    copies["down"], copies["norm"] = out[0], out[1].reshape(-1)
    codes = [code for code in range(size) if not code & 2]
    out = collect_stage([(groups[rows], only(rows, codes), codes, None)])
    late = range(size - 2)
    rest = None
    for codes, both in (
        ([code for code in late if code & 2], late), ([size - 2], [size - 2]), ([size - 1], [size - 1])
    ):
        out = collect_stage([(groups[rows], only(rows, codes), codes, out[:m]), (groups[mixed], only(mixed, both), both, rest)])
        rest = out[m:]
    for t, name in enumerate(groups[rows].members + groups[mixed].members):
        copies[name] = out[t]
    return tuple(table[name] for table in (copies, news, states) for name in names)


def fits(size, weights):
    good = size >= 4 and size & (size - 1) == 0
    for name, weight in zip(names, weights):
        good = good and weight.shape[-1] % LANES == 0
        if weight.ndim == 2:
            good = good and weight.shape[0] % 16 == 0
            if cut_dim[name] == 1:
                good = good and weight.shape[1] == LANES
        else:
            good = good and weight.shape[0] == LANES
    return good


def body(*args):
    if fits(lax.axis_size(AXIS), args[7:14]):
        return fast_body(*args)
    return plain_body(*args)


def plain_body(*args):
    size = lax.axis_size(AXIS)
    copies, news, states = [], [], []
    for name, grad, weight, moment in zip(names, args[:7], args[7:14], args[14:21]):
        dim = cut_dim.get(name, 0)
        if name in cut_dim:
            mean = lax.psum_scatter(grad[0].astype(jnp.bfloat16), AXIS, scatter_dimension=dim, tiled=True)
            mean = mean.astype(jnp.float32)
        else:
            length = weight.shape[0]
            mean = lax.dynamic_slice_in_dim(lax.psum(grad[0], AXIS), lax.axis_index(AXIS) * length, length)
        state = hold_rate * moment + mean * size ** (-0.5)
        new = weight - learn_rate * state
        copies.append(lax.all_gather(new.astype(jnp.bfloat16), AXIS, axis=dim, tiled=True))
        news.append(new)
        states.append(state)
    return tuple(copies + news + states)


def solution(mesh):
    grads, shards, wholes = [], [], []
    for name in names:
        if name not in cut_dim:
            grads.append(P(AXIS, None))
            shards.append(P(AXIS))
            wholes.append(P())
        elif cut_dim[name] == 0:
            grads.append(P(AXIS, None, COLS))
            shards.append(P(AXIS, COLS))
            wholes.append(P(None, COLS))
        else:
            grads.append(P(AXIS, COLS, None))
            shards.append(P(COLS, AXIS))
            wholes.append(P(COLS, None))
    in_specs, out_specs = tuple(grads + shards + shards), tuple(wholes + shards + shards)
    return jax.shard_map(body, mesh=mesh, in_specs=in_specs, out_specs=out_specs, check_vma=False)
```

```python
import functools

import jax
import jax.numpy as jnp
from jax import lax
from jax.experimental import pallas as pl
from jax.experimental.pallas import tpu as pltpu
from jax.sharding import PartitionSpec as P


learn_rate = 0.1
hold_rate = 0.7
AXIS, COLS = "batch", "cols"
LANES = 128
PAD = 8


names = ("up", "down", "query", "key", "value", "mixed", "norm")
cut_dim = {"up": 0, "down": 1, "query": 0, "key": 0, "value": 0, "mixed": 1}


class Plan:
    def __init__(self, steps, dim, members, shards, norm):
        self.steps, self.dim, self.members, self.norm = steps, dim, members, norm
        self.shards = shards
        self.offsets, total = [], 0
        for name in members:
            self.offsets.append(total)
            total += shards[name][1 - dim]
        first = shards[members[0]]
        total += PAD if norm else 0
        self.block = (first[0], total) if dim == 0 else (total, first[1])
        self.groups = [self]

    def part(self, t):
        rows, columns = self.shards[self.members[t]]
        start = self.offsets[t]
        if self.dim == 0:
            return (slice(None), slice(start, start + columns))
        return (slice(start, start + rows), slice(None))

    def place(self, t, owner):
        rows, columns = self.shards[self.members[t]]
        if self.dim == 0:
            return (pl.ds(pl.multiple_of(owner * rows, rows), rows), slice(None))
        return (slice(None), pl.ds(pl.multiple_of(owner * columns, columns), columns))

    def pad_row(self):
        return slice(self.block[0] - PAD, self.block[0] - PAD + 1)

    def pad(self):
        return (slice(self.block[0] - PAD, self.block[0]), slice(None))


def mask_of(code, me, steps):
    colour = (me & 1) ^ (code & 1)
    mask = code & 1
    for k in range(1, steps):
        mask = mask + ((code >> k) & 1) * ((1 << k) + colour * ((1 << (steps - k)) - (1 << k)))
    return mask


def owner_of(code, steps):
    me = lax.axis_index(AXIS)
    return me ^ mask_of(code, me, steps)


def partners(k, steps):
    pairs = []
    for me in range(1 << steps):
        if k == 0:
            bit = 0
        else:
            bit = k if me & 1 == 0 else steps - k
        pairs.append((me, me ^ (1 << bit)))
    return pairs


def exchange(x, k, steps):
    return lax.ppermute(x, AXIS, partners(k, steps))


def split_rows(x):
    high = x.astype(jnp.bfloat16).astype(jnp.float32)
    low = x - high
    row = lax.broadcasted_iota(jnp.int32, (PAD, x.shape[1]), 0)
    return jnp.where(row == 0, high, jnp.where(row == 1, low, 0.0)).astype(jnp.bfloat16)


def gathered(plan, t, own, received):
    part = (0,) + plan.part(t)
    total = own[part]
    for r in received:
        total += r[part].astype(jnp.float32)
    return total


def gathered_norm(plan, own, received):
    total = own[0, plan.pad_row(), :]
    for r in received:
        total += jnp.sum(r[(0,) + plan.pad()].astype(jnp.float32), axis=0, keepdims=True)
    return total


def send_kernel(plan, own, *refs):
    received, out = refs[:-1], refs[-1]
    for t in range(len(plan.members)):
        out[(0,) + plan.part(t)] = gathered(plan, t, own, received).astype(jnp.bfloat16)
    if plan.norm:
        out[(0,) + plan.pad()] = split_rows(gathered_norm(plan, own, received))


def first_kernel(jobs, *refs):
    inputs = []
    for plan, _, _ in jobs:
        n = len(plan.members) + int(plan.norm)
        inputs.append(refs[:n])
        refs = refs[n:]
    outs, scratches, sems = refs[: len(jobs)], refs[len(jobs) : -1], refs[-1]
    count = 0

    def fetch(plan, grads, code, target):
        nonlocal count
        owner = owner_of(code, plan.steps)
        pairs = [(grads[t].at[plan.place(t, owner)], plan.part(t)) for t in range(len(plan.members))]
        if plan.norm:
            pairs.append((grads[-1].at[:, pl.ds(pl.multiple_of(owner * LANES, LANES), LANES)], (plan.pad_row(), slice(None))))
        copies = []
        for source, part in pairs:
            copies.append(pltpu.make_async_copy(source, target.at[part], sems.at[count]))
            copies[-1].start()
            count += 1
        return copies

    landing, reads = [], []
    for (plan, codes, keep), grads, out in zip(jobs, inputs, outs):
        if keep:
            landing.append(out)
        else:
            landing.append(scratches[0])
            scratches = scratches[1:]
        reads.append([fetch(plan, grads, code, landing[-1].at[q]) for q, code in enumerate(codes)])
    for (plan, codes, keep), out, source, copies in zip(jobs, outs, landing, reads):
        for q in range(len(codes)):
            for t, copy in enumerate(copies[q]):
                copy.wait()
                if keep:
                    continue
                if t < len(plan.members):
                    out[(q,) + plan.part(t)] = source[(q,) + plan.part(t)].astype(jnp.bfloat16)
                else:
                    out[(q,) + plan.pad()] = split_rows(source[q, plan.pad_row(), :])


def first_stage(jobs):
    listed, operands, out_shape, scratch = [], [], [], []
    copies = size = 0
    for plan, (base, stride, count), grads, keep in jobs:
        shape = (count,) + plan.block
        listed.append((plan, [base + (q << stride) - int(keep) for q in range(count)], keep))
        operands += [pltpu.with_memory_space_constraint(g, pltpu.HBM) for g in grads]
        out_shape.append(jax.ShapeDtypeStruct(shape, jnp.float32 if keep else jnp.bfloat16))
        if not keep:
            scratch.append(pltpu.VMEM(shape, jnp.float32))
        copies += count * len(grads)
        size += shape[0] * shape[1] * shape[2]
    return pl.pallas_call(
        functools.partial(first_kernel, listed),
        out_shape=out_shape,
        in_specs=[pl.BlockSpec(memory_space=pl.ANY)] * len(operands),
        out_specs=[pl.BlockSpec(memory_space=pltpu.VMEM)] * len(out_shape),
        scratch_shapes=scratch + [pltpu.SemaphoreType.DMA((copies,))],
        cost_estimate=pl.CostEstimate(flops=4 * size, bytes_accessed=6 * size, transcendentals=0),
        compiler_params=pltpu.CompilerParams(vmem_limit_bytes=16 * 2**20),
    )(*operands)


def messages_of(k, steps):
    if k == steps - 1:
        return [(1 << k, k + 1, 1)]
    high = (3 << k, k + 2, 1 << (steps - 2 - k))
    low = (1 << k, k + 2, 1 << (steps - 2 - k))
    if k > 0 or steps < 3:
        return [high, low]
    half = high[2] // 2
    return [(7 << k, k + 3, half), (3 << k, k + 3, half), low]


def find(message, k, kept, received):
    base, stride, count = message
    codes = [base + (q << stride) for q in range(count)]
    places = []
    for table in [kept] + received[:k]:
        for (first, step, size), array in table:
            held = [first + (i << step) for i in range(size)]
            if all(code in held for code in codes):
                places.append((array, first, step))
                break
    return places


def send_stage(plan, k, message, kept, received):
    base, stride, count = message
    block = (1,) + plan.block
    parts, specs = [], []
    for array, first, step in find(message, k, kept, received):
        parts.append(array)
        specs.append(pl.BlockSpec(block, lambda q, first=first, step=step: ((base + (q << stride) - first) >> step, 0, 0)))
    size = count * plan.block[0] * plan.block[1]
    return pl.pallas_call(
        functools.partial(send_kernel, plan),
        grid=(count,),
        out_shape=jax.ShapeDtypeStruct((count,) + plan.block, jnp.bfloat16),
        in_specs=specs,
        out_specs=pl.BlockSpec(block, lambda q: (q, 0, 0)),
        cost_estimate=pl.CostEstimate(flops=4 * size, bytes_accessed=(6 + 2 * k) * size, transcendentals=0),
        compiler_params=pltpu.CompilerParams(vmem_limit_bytes=16 * 2**20),
    )(*parts)


def update_kernel(plan, rate, *refs):
    m = len(plan.members)
    n = m + int(plan.norm)
    own, received, refs = refs[0], refs[1 : 1 + plan.steps], refs[1 + plan.steps :]
    weights, moments, refs = refs[:n], refs[n : 2 * n], refs[2 * n :]
    copies, refs = refs[: len(plan.groups)], refs[len(plan.groups) :]
    new, state = refs[:n], refs[n:]
    for t in range(n):
        if t < m:
            mean = gathered(plan, t, own, received) * rate
        else:
            mean = gathered_norm(plan, own, received) * rate
        held = hold_rate * moments[t][...] + mean
        fresh = weights[t][...] - learn_rate * held
        state[t][...] = held
        new[t][...] = fresh
        for group, copy in zip(plan.groups, copies):
            if t == m:
                if group.norm:
                    copy[(0,) + group.pad()] = split_rows(fresh)
            elif plan.members[t] in group.members:
                place = group.part(group.members.index(plan.members[t]))
                copy[(0,) + place] = fresh.astype(jnp.bfloat16)


def update_stage(plan, kept, received, weights, moments):
    block = (1,) + plan.block
    parts = [array for array, _, _ in find((0, 0, 1), plan.steps, kept, received)]
    specs = [pl.BlockSpec(block, lambda q: (0, 0, 0)) for _ in parts]
    shards = [plan.shards[name] for name in plan.members]
    if plan.norm:
        shards.append((1, plan.shards["norm"]))
    whole = [pl.BlockSpec(shape, lambda q: (0, 0)) for shape in shards]
    arrays = [jax.ShapeDtypeStruct(shape, jnp.float32) for shape in shards]
    copies = [(1,) + group.block for group in plan.groups]
    size = plan.block[0] * plan.block[1]
    n, m = len(shards), len(copies)
    out = pl.pallas_call(
        functools.partial(update_kernel, plan, (1 << plan.steps) ** (-0.5)),
        grid=(1,),
        out_shape=[jax.ShapeDtypeStruct(shape, jnp.bfloat16) for shape in copies] + arrays + arrays,
        in_specs=specs + whole + whole,
        out_specs=[pl.BlockSpec(shape, lambda q: (0, 0, 0)) for shape in copies] + whole + whole,
        cost_estimate=pl.CostEstimate(flops=12 * size, bytes_accessed=28 * size, transcendentals=0),
        compiler_params=pltpu.CompilerParams(vmem_limit_bytes=24 * 2**20),
    )(*parts, *weights, *moments)
    return out[:m], out[m : m + n], out[m + n :]


def collect_kernel(jobs, aliased, *refs):
    inputs = sum(len(codes) for _, codes, _ in jobs)
    pieces, refs = refs[:inputs], refs[inputs + aliased :]
    writes, norms = [], []
    outs, count = refs, 0
    for plan, _, _ in jobs:
        count += len(plan.members) + int(plan.norm)
    outs, scratch = refs[:count], refs[count:]
    sems = scratch[0]
    for plan, codes, fresh in jobs:
        m = len(plan.members)
        held, pieces = dict(zip(codes, pieces)), pieces[len(codes) :]
        targets, outs = outs[: m + int(plan.norm)], outs[m + int(plan.norm) :]
        if plan.norm:
            rows, row_sems, table = scratch[1:]
            reads = []
            for p, code in enumerate(codes):
                reads.append(pltpu.make_async_copy(held[code].at[(0,) + plan.pad()], rows.at[p], row_sems.at[p]))
                reads[-1].start()
            norms.append((plan, codes, reads, targets[-1]))
        for code in fresh:
            owner = owner_of(code, plan.steps)
            for t in range(m):
                place = plan.place(t, owner)
                source = held[code].at[(0,) + plan.part(t)]
                writes.append(pltpu.make_async_copy(source, targets[t].at[place], sems.at[len(writes)]))
                writes[-1].start()
    for plan, codes, reads, target in norms:
        for p, code in enumerate(codes):
            reads[p].wait()
            row = jnp.sum(rows[p].astype(jnp.float32), axis=0, keepdims=True)
            table[pl.ds(owner_of(code, plan.steps), 1), :] = row
        target[...] = table[...].astype(jnp.bfloat16)
    for w in writes:
        w.wait()


def collect_stage(jobs):
    operands, filled, out_shape, out_specs, aliases = [], [], [], [], {}
    scratch, copies, moved = [], 0, 0
    inputs = sum(len(pieces) for _, pieces, _, _ in jobs)
    for plan, pieces, fresh, rest in jobs:
        operands += list(pieces.values())
        copies += len(fresh) * len(plan.members)
        moved += len(fresh) * plan.block[0] * plan.block[1]
        size = 1 << plan.steps
        for t, name in enumerate(plan.members):
            rows, columns = plan.shards[name]
            if rest is not None:
                aliases[inputs + len(filled)] = len(out_shape)
                filled.append(rest[t])
            shape = (rows * size, columns) if plan.dim == 0 else (rows, columns * size)
            out_shape.append(jax.ShapeDtypeStruct(shape, jnp.bfloat16))
            out_specs.append(pl.BlockSpec(memory_space=pltpu.HBM))
        if plan.norm:
            width = plan.shards["norm"]
            out_shape.append(jax.ShapeDtypeStruct((size, width), jnp.bfloat16))
            out_specs.append(pl.BlockSpec(memory_space=pltpu.VMEM))
            scratch = [
                pltpu.VMEM((len(pieces), PAD, width), jnp.bfloat16),
                pltpu.SemaphoreType.DMA((len(pieces),)),
                pltpu.VMEM((size, width), jnp.float32),
            ]
    listed = tuple((plan, tuple(pieces), tuple(fresh)) for plan, pieces, fresh, _ in jobs)
    return pl.pallas_call(
        functools.partial(collect_kernel, listed, len(filled)),
        out_shape=out_shape,
        in_specs=[pl.BlockSpec(memory_space=pl.ANY)] * (inputs + len(filled)),
        out_specs=out_specs,
        scratch_shapes=[pltpu.SemaphoreType.DMA((copies,))] + scratch,
        input_output_aliases=aliases,
        cost_estimate=pl.CostEstimate(flops=4 * moved, bytes_accessed=4 * moved, transcendentals=0),
        compiler_params=pltpu.CompilerParams(vmem_limit_bytes=4 * 2**20),
    )(*operands, *filled)


def fast_body(*args):
    grads = dict(zip(names, args[:7]))
    weights = dict(zip(names, args[7:14]))
    moments = dict(zip(names, args[14:21]))
    size = lax.axis_size(AXIS)
    steps = size.bit_length() - 1
    shards = {name: weights[name].shape for name in names[:-1]}
    shards["norm"] = weights["norm"].shape[0]
    plans = (
        Plan(steps, 1, ("down", "mixed"), shards, True),
        Plan(steps, 0, ("up", "query", "key", "value"), shards, False),
    )
    plans[0].groups = [Plan(steps, 1, ("down",), shards, True), Plan(steps, 1, ("mixed",), shards, False)]
    plans[1].groups = [Plan(steps, 0, ("up",), shards, False), Plan(steps, 0, ("query", "key", "value"), shards, False)]

    def inputs(plan, arrays, squeeze):
        out = [arrays[name][0] if squeeze else arrays[name] for name in plan.members]
        if plan.norm:
            out.append(arrays["norm"] if squeeze else arrays["norm"].reshape(1, -1))
        return out

    g = [inputs(plan, grads, True) for plan in plans]
    received = [[[] for _ in range(steps)] for _ in plans]
    kept = [[] for _ in plans]
    stage = messages_of(0, steps)
    for i, message in enumerate(stage):
        for c, plan in enumerate(plans):
            own = [(c, message)]
            if i == 0:
                own = [] if c == 0 else [(0, message)]
            elif i == 1:
                own = [(1, stage[0])] if c == 0 else [(0, message), (1, message)]
            jobs = [(plan, message, g[c], False)] + [(plans[d], which, g[d], True) for d, which in own]
            sent, *rest = first_stage(jobs)
            for (d, (base, stride, count)), array in zip(own, rest):
                kept[d].append(((base - 1, stride, count), array))
            received[c][0].append(((message[0] - 1,) + message[1:], exchange(sent, 0, steps)))
    for k in range(1, steps):
        for message in messages_of(k, steps):
            for c, plan in enumerate(plans):
                sent = send_stage(plan, k, message, kept[c], received[c])
                received[c][k].append(((message[0] - (1 << k),) + message[1:], exchange(sent, k, steps)))
    copies, news, states = {}, {}, {}
    groups, pieces = [], []
    for c, plan in enumerate(plans):
        fresh, new, state = update_stage(
            plan, kept[c], received[c], inputs(plan, weights, False), inputs(plan, moments, False)
        )
        members = plan.members + (("norm",) if plan.norm else ())
        for name, a, b in zip(members, new, state):
            news[name] = a.reshape(weights[name].shape)
            states[name] = b.reshape(weights[name].shape)
        groups += plan.groups
        pieces += [{0: x} for x in fresh]
    for k in reversed(range(steps)):
        for i, held in enumerate(pieces):
            for code, x in list(held.items()):
                if i == 1 and k == 0 and code == size - 2:
                    pairs = [(me, other ^ 1) for me, other in partners(1, steps)]
                    held[size - 1] = lax.ppermute(held[size - 4], AXIS, pairs)
                else:
                    held[code | 1 << k] = exchange(x, k, steps)

    def job(i, codes, rest):
        return groups[i], {code: pieces[i][code] for code in codes}, codes, rest

    late = range(size - 2)
    bare = Plan(steps, 1, groups[0].members, shards, False)
    out = collect_stage([(bare, {code: pieces[0][code] for code in late}, late, None)])
    out = collect_stage([(groups[0], pieces[0], [size - 2, size - 1], out)])
    copies.update(zip(groups[0].members, out))
    copies["norm"] = out[-1].reshape(-1)
    ups = collect_stage([job(2, [code for code in range(size) if not code & 2], None)])
    out = collect_stage([job(2, [code for code in late if code & 2], ups), job(3, late, None), job(1, late, None)])
    ups, rest, small = out[:1], out[1:-1], out[-1:]
    out = collect_stage([job(2, [size - 2], ups), job(3, [size - 2], rest)])
    ups, rest = out[:1], out[1:]
    out = collect_stage([job(2, [size - 1], ups), job(3, [size - 1], rest), job(1, [size - 2, size - 1], small)])
    ups, rest, small = out[:1], out[1:-1], out[-1:]
    for i, arrays in ((1, small), (2, ups), (3, rest)):
        copies.update(zip(groups[i].members, arrays))
    return tuple(table[name] for table in (copies, news, states) for name in names)


def fits(size, weights):
    good = size >= 4 and size & (size - 1) == 0
    for name, weight in zip(names, weights):
        good = good and weight.shape[-1] % LANES == 0
        if weight.ndim == 2:
            good = good and weight.shape[0] % 16 == 0
            if cut_dim[name] == 1:
                good = good and weight.shape[1] == LANES
        else:
            good = good and weight.shape[0] == LANES
    return good


def body(*args):
    if fits(lax.axis_size(AXIS), args[7:14]):
        return fast_body(*args)
    return plain_body(*args)


def plain_body(*args):
    size = lax.axis_size(AXIS)
    copies, news, states = [], [], []
    for name, grad, weight, moment in zip(names, args[:7], args[7:14], args[14:21]):
        dim = cut_dim.get(name, 0)
        if name in cut_dim:
            mean = lax.psum_scatter(grad[0].astype(jnp.bfloat16), AXIS, scatter_dimension=dim, tiled=True)
            mean = mean.astype(jnp.float32)
        else:
            length = weight.shape[0]
            mean = lax.dynamic_slice_in_dim(lax.psum(grad[0], AXIS), lax.axis_index(AXIS) * length, length)
        state = hold_rate * moment + mean * size ** (-0.5)
        new = weight - learn_rate * state
        copies.append(lax.all_gather(new.astype(jnp.bfloat16), AXIS, axis=dim, tiled=True))
        news.append(new)
        states.append(state)
    return tuple(copies + news + states)


def solution(mesh):
    grads, shards, wholes = [], [], []
    for name in names:
        if name not in cut_dim:
            grads.append(P(AXIS, None))
            shards.append(P(AXIS))
            wholes.append(P())
        elif cut_dim[name] == 0:
            grads.append(P(AXIS, None, COLS))
            shards.append(P(AXIS, COLS))
            wholes.append(P(None, COLS))
        else:
            grads.append(P(AXIS, COLS, None))
            shards.append(P(COLS, AXIS))
            wholes.append(P(COLS, None))
    in_specs, out_specs = tuple(grads + shards + shards), tuple(wholes + shards + shards)
    return jax.shard_map(body, mesh=mesh, in_specs=in_specs, out_specs=out_specs, check_vma=False)
```
